32 devices in a mesh: tm: 8 (over y, x, core), tx: 4 (over z).
Axes of the slice: x: 2, y: 2, z: 4, core: 2. Of those that a mesh axis runs over, the one named last changes fastest.
Arguments:
- state: float32 [8, 64, 256, 128], P('tm', 'tx'), may hold values from -6 to 6
- force: float32 [8, 64, 256, 128], P('tm', 'tx'), may hold values from -6 to 6
- u_init: float32 [64, 256, 128], P('tx'), may hold values from -6 to 6
- kappa: float32 [64, 256], P('tx'), may hold values from 0.1 to 2
- rates: float32 [128], replicated, may hold values from 0.05 to 4
- basis: float32 [128, 128], replicated, may hold values from -1 to 1, as said below
Outputs:
- correction: float32 [8, 64, 256, 128], P('tm', 'tx')
The draws below stay inside these ranges and needn't reach their ends.
Inputs may be any that keep to these rules, and one draw needn't show every extreme that they name: basis is an orthogonal matrix.
All inputs are finite; a program needn't handle non-finite values.
Results may differ from the reference program's by a relative error of at most 0.0003.
Values sent between devices are 32-bit elements; how exact they have to be, the bound alone decides.
No kernel may reach another device: no remote copies, remote signals or barrier semaphores. Data moves between devices by JAX's collectives and lax.ppermute only.
A program may use at most 64 MiB of HBM per device.

```python
import math
import jax
import jax.numpy as jnp
from jax import lax

K = 128
NY = 256
NX = 64
NT = 8


def draw_basis(key, part):
    raw = jax.random.normal(key, (K, K), jnp.float32)
    ortho, upper = jnp.linalg.qr(raw)
    return ortho.astype(jnp.float32)


def steps_of(stream_key, shape, pieces, low, high):
    loudness, own = 1.0, jax.random.fold_in(stream_key, 6)
    for dim, blocks in pieces:
        draws = jnp.exp(jax.random.uniform(jax.random.fold_in(own, dim), (blocks,), jnp.float32, low / len(pieces), high / len(pieces)))
        loudness = loudness * jnp.repeat(draws, shape[dim] // blocks).reshape([-1 if axis == dim else 1 for axis in range(len(shape))])
    return loudness


def noise(stream_key, extent, spread, limit, split=(), held_as=jnp.bfloat16):
    entries = spread * jax.random.normal(stream_key, extent, jnp.float32)
    if split:
        entries = entries * steps_of(stream_key, extent, split, -0.22, 0.18)
    return jnp.clip(entries, -limit, limit).astype(held_as)


def setup_inputs(seed: int = 0) -> dict:
    splits = jax.random.split(jax.random.key(seed), 7)
    state = noise(splits[0], (NT, NX, NY, K), 1.0, 6.0, ((0, 8), (1, 4)), jnp.float32)
    force = noise(splits[1], (NT, NX, NY, K), 1.0, 6.0, ((0, 8), (1, 4)), jnp.float32)
    u_init = noise(splits[2], (NX, NY, K), 1.0, 6.0, ((0, 4),), jnp.float32)
    kappa = jnp.clip(jnp.exp(math.log(2.0) - 2.9957323 * jax.random.uniform(splits[3], (NX, NY), jnp.float32) ** steps_of(splits[3], (NX, NY), ((0, 4),), -0.2, 0.2)), 0.1, 2.0)
    rates = jnp.clip(jnp.exp(jax.random.uniform(splits[4], (K,), jnp.float32, math.log(0.05), math.log(4.0))), 0.05, 4.0)
    basis = draw_basis(jax.random.fold_in(splits[6], 71), 0)
    return {"state": state, "force": force, "u_init": u_init, "kappa": kappa, "rates": rates, "basis": basis}


ALPHA = 0.05
TWO_PI = 2.0 * math.pi

def neighbours(field):
    widths = [(0, 0)] * (field.ndim - 3) + [(1, 1), (1, 1), (0, 0)]
    padded = jnp.pad(field, widths)
    return padded[..., 2:, 1:-1, :] + padded[..., :-2, 1:-1, :] + padded[..., 1:-1, 2:, :] + padded[..., 1:-1, :-2, :]

def reference(state, force, u_init, kappa, rates, basis):
    highest = lax.Precision.HIGHEST
    earlier = jnp.concatenate([u_init[None], state[:-1]], axis=0)
    coords = jnp.dot(state.reshape(-1, K), basis, precision=highest)
    vertical = jnp.dot(coords * rates, basis.T, precision=highest).reshape(state.shape)
    kappa_b = kappa[None, :, :, None]
    residual = force - (state - earlier) - vertical - kappa_b * (4.0 * state - neighbours(state)) - 0.5 * state ** 3 / (1.0 + state * state)
    modal = jnp.dot(residual.reshape(-1, K), basis, precision=highest).reshape(state.shape)
    indices = jnp.arange(NT)
    steps_f = indices.astype(jnp.float32)
    decay = jnp.log(ALPHA) / NT
    scaled = modal * jnp.exp(decay * steps_f)[:, None, None, None]
    products = (indices[:, None] * indices[None, :] % NT).astype(jnp.float32)
    angles = TWO_PI * products / NT
    cosine = jnp.cos(angles)
    sine = jnp.sin(angles)
    flat_cells = scaled.reshape(NT, -1)
    spec_re = jnp.dot(cosine, flat_cells, precision=highest).reshape(state.shape)
    spec_im = -jnp.dot(sine, flat_cells, precision=highest).reshape(state.shape)
    factor = jnp.exp(decay)
    theta = TWO_PI * steps_f / NT
    real_den = (1.0 - factor * jnp.cos(theta))[:, None, None, None] + rates + 4.0 * kappa_b
    imag_den = (factor * jnp.sin(theta))[:, None, None, None] + jnp.zeros_like(real_den)
    magnitude = real_den * real_den + imag_den * imag_den

    def divide(num_re, num_im):
        return ((num_re * real_den + num_im * imag_den) / magnitude, (num_im * real_den - num_re * imag_den) / magnitude)
    field_re, field_im = divide(spec_re, spec_im)
    for repeat in range(2):
        field_re, field_im = divide(spec_re + kappa_b * neighbours(field_re), spec_im + kappa_b * neighbours(field_im))
    flat_re = field_re.reshape(NT, -1)
    flat_im = field_im.reshape(NT, -1)
    times = (jnp.dot(cosine, flat_re, precision=highest) - jnp.dot(sine, flat_im, precision=highest)) / NT
    times = times * jnp.exp(-decay * steps_f)[:, None]
    back = times.reshape(state.shape)
    return jnp.dot(back.reshape(-1, K), basis.T, precision=highest).reshape(state.shape)
```

```python
import functools

import jax
import jax.numpy as jnp
from jax import lax
from jax.experimental import pallas as pl
from jax.experimental.pallas import tpu as pltpu
from jax.sharding import PartitionSpec as P


ALPHA = 0.05
REACH = 2
F32 = jnp.float32
BF16 = jnp.bfloat16
MIB = 2**20


def split(value):
    high = value.astype(BF16)
    return high, (value - high.astype(F32)).astype(BF16)


def dot(left, right):
    return jnp.dot(left, right, preferred_element_type=F32)


def shifted(array, axis, by):
    count = lax.axis_size(axis)
    pairs = [(i, i + by) for i in range(count) if 0 <= i + by < count]
    return lax.ppermute(array, axis, pairs)


def cut(value, rows, out, base, blocks):
    size = value.shape[0]
    block = size // blocks
    tall = block + 2 * REACH
    rows[pl.ds(REACH, size), :] = value
    for target in range(blocks):
        out[target, pl.ds(base, tall), :] = rows[pl.ds(block * target, tall), :]


def fill_weights(weights, first_half, second_half):
    depth = first_half.shape[0]
    first_high, first_low = split(first_half)
    weights[:depth, :depth] = first_high
    weights[:depth, depth:] = first_low
    if second_half is None:
        weights[depth:, :depth] = first_high
        weights[depth:, depth:] = jnp.zeros_like(first_low)
    else:
        second_high, second_low = split(second_half)
        weights[depth:, :depth] = second_high
        weights[depth:, depth:] = second_low


def times_matrix(value, weights):
    depth = value.shape[1]
    wide = dot(jnp.concatenate(split(value), axis=1), weights[...])
    return wide[:, :depth] + wide[:, depth:]


def residual_kernel(
    blocks, inner, state, other, initial, force, low, high, kappa, rates, basis, out,
    here, past, pushed, parts, rows, levels, turned, weights, loads, stores,
):
    columns, size, depth = state.shape
    tall = size // blocks + 2 * REACH
    step_here = lax.axis_index("tm")
    odd = step_here % 2 == 1
    first = step_here == 0
    if inner:
        mine = list(range(2, columns - 2))
        wide = list(range(1, columns - 1))
    else:
        mine = [0, 1, columns - 2, columns - 1]
        wide = [0, 1, 2, columns - 3, columns - 2, columns - 1]

    def load(kind, x):
        source, target = ((state, here), (other, past), (force, pushed))[kind]
        return pltpu.make_async_copy(source.at[x], target.at[x], loads.at[kind, x])

    for x in wide:
        load(0, x).start()
        if x in mine:
            load(2, x).start()

            @pl.when(odd)
            def _():
                load(1, x).start()

            @pl.when(first)
            def _():
                pltpu.make_async_copy(initial.at[x], past.at[x], loads.at[1, x]).start()

    plain = basis[...]
    fill_weights(weights, plain, -plain * rates[...])
    rows[...] = jnp.zeros_like(rows)
    index = lax.broadcasted_iota(jnp.int32, (size, depth), 0)
    levels[...] = jnp.zeros_like(levels)
    levels[:columns, :] = kappa[...]
    for part in range(size // depth):
        where = pl.ds(part * depth, depth)
        turned[where, :] = jnp.transpose(levels[:, where])

    def column(x, left, right, base):
        load(2, x).wait()

        @pl.when(jnp.logical_or(odd, first))
        def _():
            load(1, x).wait()

        center = here[x]
        up = jnp.where(index == 0, 0.0, pltpu.roll(center, 1, 0))
        down = jnp.where(index == size - 1, 0.0, pltpu.roll(center, size - 1, 0))
        square = center * center
        beside = left + right + up + down
        across = jnp.broadcast_to(pltpu.roll(turned[...], (depth - x) % depth, 1)[:, :1], (size, depth))
        value = (
            pushed[x]
            - center
            + jnp.where(jnp.logical_or(odd, first), past[x], 0.0)
            - across * (4.0 * center - beside)
            - 0.5 * (square * center) / (1.0 + square)
        )
        value_high, value_low = split(value)
        center_high, center_low = split(center)
        joined_high = jnp.concatenate([value_high, center_high], axis=1)
        joined_low = jnp.concatenate([value_low, center_low], axis=1)
        product = dot(joined_high, weights[...])
        modal = product[:, :depth] + product[:, depth:] + dot(joined_low, weights[:, :depth])
        cut(modal, rows, parts, base, blocks)

    def store(step):
        where = pl.ds(pl.multiple_of(step * 2 * tall, 8), 2 * tall)
        return pltpu.make_async_copy(parts.at[:, where, :], out.at[:, where, :], stores.at[step])

    if inner:
        load(0, 1).wait()
        load(0, 2).wait()

        def pair(step, carry):
            base = pl.multiple_of(step * 2 * tall, 8)
            for which in range(2):
                x = 2 + 2 * step + which
                load(0, x + 1).wait()
                column(x, here[x - 1], here[x + 1], base + which * tall)
            store(step).start()
            return carry

        lax.fori_loop(0, len(mine) // 2, pair, 0)
    else:
        for x in wide:
            load(0, x).wait()
        column(0, low[:size, :], here[1], 0)
        column(1, here[0], here[2], tall)
        store(0).start()
        column(columns - 2, here[columns - 3], here[columns - 1], 2 * tall)
        column(columns - 1, here[columns - 2], high[:size, :], 3 * tall)
        store(1).start()
    for step in range(len(mine) // 2):
        store(step).wait()


def prepare_kernel(
    block, count, edge, state, other, kappa, rates, basis, *rest
):
    pieces, shared = rest[:count], rest[count : 2 * count]
    modal, inverse, ending, low, high, near, far, strip, gathered, weights, loads = rest[2 * count :]
    columns, window, depth = far.shape[1:]
    broad = near.shape[1]
    chips = count + 1
    steps = 2 * chips
    size = block * steps
    tall = block + 2 * REACH
    two = REACH * tall
    room = (strip.shape[0] - broad) // 2
    here = lax.axis_index("tm")
    chip = here // 2
    odd = here % 2 == 1
    near_start = pl.multiple_of(near_begin(chip, block, broad, size), 8)

    @pl.when(odd)
    def _():
        pltpu.make_async_copy(state.at[:, pl.ds(near_start, broad), :], near, loads.at[count]).start()
        for by in range(count):
            pltpu.make_async_copy(pieces[by], far.at[by], loads.at[by]).start()

    @pl.when(jnp.logical_not(odd))
    def _():
        pltpu.make_async_copy(other.at[:, pl.ds(near_start, broad), :], near, loads.at[count]).start()
        for by in range(count):
            pltpu.make_async_copy(shared[by], far.at[by], loads.at[by]).start()

    fill_weights(weights, basis[...], None)
    total = kappa.shape[0]
    chunk = 2 * tall

    def factors(step, carry):
        base = pl.multiple_of(step * chunk, 8)
        inv = 1.0 / (1.0 + rates[...] + 4.0 * kappa[pl.ds(base, chunk), :])
        inverse[pl.ds(base, chunk), :] = inv
        power = inv
        for _ in range(steps - 1):
            power = power * inv
        ending[pl.ds(base, chunk), :] = ALPHA / (1.0 - ALPHA * power)
        return carry

    lax.fori_loop(0, total // chunk, factors, 0)
    strip[...] = jnp.zeros_like(strip)
    begin = block * here - REACH + room

    def slot(source, start, extent, index):
        strip[room + extent :, :] = jnp.zeros((strip.shape[0] - room - extent, depth), F32)
        for x in range(columns):
            strip[pl.ds(room, extent), :] = source(x)
            gathered[pl.ds(x * tall, tall), :] = strip[pl.ds(begin - start, tall), :]
        modal[index] = times_matrix(gathered[...], weights)

    pltpu.make_async_copy(state.at[:, pl.ds(near_start, broad), :], near, loads.at[count]).wait()
    slot(lambda x: near[x], near_start, broad, chip)
    far_start = window_start(chip, block, window, size)

    def far_slot(by, carry):
        pltpu.make_async_copy(pieces[0], far.at[by], loads.at[by]).wait()
        slot(lambda x: far[by, x], far_start, window, (chip - by - 1 + chips) % chips)
        return carry

    lax.fori_loop(0, count, far_slot, 0)
    whole = columns * tall
    for n in range(steps):
        left = edge[n, :two, :]
        right = edge[n, two:, :]
        if n and n % 2 == 0:
            left = left + modal[n // 2 - 1, :two, :]
            right = right + modal[n // 2 - 1, whole - two :, :]
        low[n] = left
        high[n] = right


def relax_kernel(
    block, middle, edge_low, edge_high, left, right, modal_far, kappa_far, inverse_far, ending_far, basis, out,
    known, source, older, newer, gathered, weights, modal, kappa, inverse, ending, made_out, loads, stores,
):
    steps, inner, depth = middle.shape
    tall = block + 2 * REACH
    chunk = REACH * tall
    columns = inner // tall + 2 * REACH
    total = inner + 4 * chunk
    pad = older.shape[1] - total
    front = pad // 2
    copies = [
        (inverse_far, inverse),
        (ending_far, ending),
        (left, known.at[:, pl.ds(0, chunk), :]),
        (edge_low, known.at[:, pl.ds(chunk, chunk), :]),
        (edge_high, known.at[:, pl.ds(total - 2 * chunk, chunk), :]),
        (right, known.at[:, pl.ds(total - chunk, chunk), :]),
        (modal_far, modal),
        (kappa_far, kappa),
        (middle, known.at[:, pl.ds(2 * chunk, inner), :]),
    ]
    copies = [pltpu.make_async_copy(*ends, loads.at[i]) for i, ends in enumerate(copies)]
    for copy in copies:
        copy.start()
    fill_weights(weights, jnp.transpose(basis[...]), None)
    older[:, :front, :] = jnp.zeros((steps, front, depth), F32)
    older[:, front + total :, :] = jnp.zeros((steps, pad - front, depth), F32)

    def solve(values, inv, end):
        last = values(0) * inv
        for n in range(1, steps):
            last = (values(n) + last) * inv
        return end * last

    def first(value, base):
        inv = inverse[pl.ds(base, chunk), :]
        run = solve(value, inv, ending[pl.ds(base, chunk), :])
        for n in range(steps):
            run = (known[n, pl.ds(base, chunk), :] + run) * inv
            older[n, pl.ds(base + front, chunk), :] = run

    for copy in copies:
        copy.wait()
    for base in (0, chunk, total - 2 * chunk, total - chunk):
        first(lambda n: known[n, pl.ds(base, chunk), :], base)

    def first_middle(step, carry):
        at = pl.multiple_of(step * chunk, 8)
        base = pl.multiple_of(at + 2 * chunk, 8)

        def value(n):
            made = known[n, pl.ds(base, chunk), :]
            if n and n % 2 == 0:
                made = made + modal[n // 2 - 1, pl.ds(at + chunk, chunk), :]
                known[n, pl.ds(base, chunk), :] = made
            return made

        first(value, base)
        return carry

    lax.fori_loop(0, inner // chunk, first_middle, 0)

    def term(field, base, size, n):
        beside = (
            field[n, pl.ds(base + front - 1, size), :]
            + field[n, pl.ds(base + front + 1, size), :]
            + field[n, pl.ds(base + front - tall, size), :]
            + field[n, pl.ds(base + front + tall, size), :]
        )
        return known[n, pl.ds(base, size), :] + kappa[pl.ds(base, size), :] * beside

    def second(step, carry):
        base = pl.multiple_of(step * chunk, 8) + tall
        inv = inverse[pl.ds(base, chunk), :]

        def value(n):
            made = term(older, base, chunk, n)
            source[n, :chunk, :] = made
            return made

        run = solve(value, inv, ending[pl.ds(base, chunk), :])
        for n in range(steps):
            run = (source[n, :chunk, :] + run) * inv
            newer[n, pl.ds(base + front, chunk), :] = run
        return carry

    lax.fori_loop(0, (columns + 2) // 2, second, 0)

    def third(base):
        inv = inverse[pl.ds(base, block), :]

        def value(n):
            made = term(newer, base, block, n)
            source[n, :block, :] = made
            return made

        run = solve(value, inv, ending[pl.ds(base, block), :])
        for n in range(steps):
            run = (source[n, :block, :] + run) * inv
            gathered[pl.ds(n * block, block), :] = run
        gathered[...] = times_matrix(gathered[...], weights)

    def third_pair(step, carry):
        at = pl.multiple_of(step * 2 * tall, 8)
        to = pl.multiple_of(step * 2 * block, 8)
        for which in range(2):
            third(at + chunk + which * tall + REACH)
            for n in range(steps):
                made_out[n, pl.ds(to + which * block, block), :] = gathered[pl.ds(n * block, block), :]
        store(step).start()
        return carry

    def store(step):
        where = pl.ds(pl.multiple_of(step * 2 * block, 8), 2 * block)
        return pltpu.make_async_copy(made_out.at[:, where, :], out.at[:, where, :], stores.at[step])

    lax.fori_loop(0, columns // 2, third_pair, 0)
    for step in range(columns // 2):
        store(step).wait()


SPACES = {"v": pltpu.VMEM, "h": pltpu.HBM}


def call(kernel, outs, spaces, scratch, flops, *operands):
    shapes = [jax.ShapeDtypeStruct(shape, F32) for shape, _ in outs]
    return pl.pallas_call(
        kernel,
        out_shape=shapes,
        in_specs=[pl.BlockSpec(memory_space=SPACES[space]) for space in spaces],
        out_specs=[pl.BlockSpec(memory_space=SPACES[space]) for _, space in outs],
        scratch_shapes=scratch,
        cost_estimate=pl.CostEstimate(flops=flops, bytes_accessed=10**6, transcendentals=0),
        compiler_params=pltpu.CompilerParams(vmem_limit_bytes=60 * MIB),
    )(*operands)


def paired(array, odd_only=False):
    count = lax.axis_size("tm")
    return lax.ppermute(array, "tm", [(i, i ^ 1) for i in range(count) if i % 2 or not odd_only])


def exchanged(array):
    return lax.all_to_all(array, "tm", split_axis=0, concat_axis=0, tiled=True)


def window_start(chip, block, window, size):
    return jnp.clip(2 * block * chip - 4, 0, size - window)


def near_begin(chip, block, broad, size):
    return jnp.clip(2 * block * chip - 8, 0, size - broad)


def spread(mine, chip, chips, block, window, by):
    start = window_start((chip + by) % chips, block, window, mine.shape[1])
    rows = lax.dynamic_slice_in_dim(mine, start, window, 1)
    count = 2 * chips
    return lax.ppermute(rows, "tm", [(i, (i + 2 * by) % count) for i in range(1, count - 1, 2)])


def correction(state, force, u_init, kappa, rates, basis):
    steps = lax.axis_size("tm")
    here = lax.axis_index("tm")
    chips = steps // 2
    chip = here // 2
    columns, size, depth = u_init.shape
    block = size // steps
    tall = block + 2 * REACH
    chunk = REACH * tall
    window = 2 * block + 8
    broad = 2 * block + 16
    total = columns * tall + 2 * chunk
    front = (tall + 15) // 8 * 8
    square = pltpu.VMEM((2 * depth, 2 * depth), BF16)
    mine = state[0]
    other = paired(mine)
    folded = kappa.reshape(columns, size // depth, depth)
    room = jnp.zeros((-(REACH * size // depth) % 8, depth), F32)

    def bundle(column, coefficients):
        return jnp.concatenate([column, coefficients.reshape(-1, depth), room], axis=0)

    low = shifted(bundle(mine[-1], folded[-REACH:]), "tx", 1)
    high = shifted(bundle(mine[0], folded[:REACH]), "tx", -1)
    rates_row = rates.reshape(1, depth)
    pieces = []
    for by in range(1, chips):
        pieces.append(spread(mine, chip, chips, block, window, by))

    def residual(inner, count, flops):
        return call(
            functools.partial(residual_kernel, steps, inner),
            [((steps, count * tall, depth), "h")],
            "hhhhvvvvv",
            [
                pltpu.VMEM(u_init.shape, F32),
                pltpu.VMEM(u_init.shape, F32),
                pltpu.VMEM(u_init.shape, F32),
                pltpu.VMEM((steps, count * tall, depth), F32),
                pltpu.VMEM((size + 8, depth), F32),
                pltpu.VMEM((depth, size), F32),
                pltpu.VMEM((size, depth), F32),
                square,
                pltpu.SemaphoreType.DMA((3, columns)),
                pltpu.SemaphoreType.DMA((count // 2,)),
            ],
            flops,
            mine, other, u_init, force[0], low, high, kappa, rates_row, basis,
        )[0]

    edge = residual(False, 2 * REACH, 2 * 10**9)
    edge = exchanged(edge)
    middle = residual(True, columns - 2 * REACH, 6 * 10**9)
    middle = exchanged(middle)
    shared = []
    for by in range(1, chips):
        shared.append(paired(pieces[by - 1], odd_only=True))
    ends = [array[size : size + REACH * size // depth].reshape(REACH, size) for array in (low, high)]
    kappa_wide = jnp.pad(jnp.concatenate([ends[0], kappa, ends[1]], axis=0), ((0, 0), (REACH, REACH)))
    kappa_mine = lax.dynamic_slice_in_dim(kappa_wide, here * block, tall, 1)
    kappa_cells = jnp.broadcast_to(kappa_mine[:, :, None], kappa_mine.shape + (depth,)).reshape(-1, depth)
    modal, inverse, ending, edge_low, edge_high = call(
        functools.partial(prepare_kernel, block, chips - 1),
        [
            ((chips, columns * tall, depth), "v"),
            ((total, depth), "v"),
            ((total, depth), "v"),
            ((steps, chunk, depth), "v"),
            ((steps, chunk, depth), "v"),
        ],
        "vhhvvv" + "h" * (2 * chips - 2),
        [
            pltpu.VMEM((columns, broad, depth), F32),
            pltpu.VMEM((chips - 1, columns, window, depth), F32),
            pltpu.VMEM((broad + 16, depth), F32),
            pltpu.VMEM((columns * tall, depth), F32),
            square,
            pltpu.SemaphoreType.DMA((chips,)),
        ],
        10**9,
        edge, mine, other, kappa_cells, rates_row, basis, *pieces, *shared,
    )
    left = shifted(edge_high, "tx", 1)
    right = shifted(edge_low, "tx", -1)
    back = call(
        functools.partial(relax_kernel, block),
        [((steps, columns * block, depth), "h")],
        "hhhhhhhhhv",
        [
            pltpu.VMEM((steps, total, depth), F32),
            pltpu.VMEM((steps, chunk, depth), F32),
            pltpu.VMEM((steps, total + 2 * front, depth), F32),
            pltpu.VMEM((steps, total + 2 * front, depth), F32),
            pltpu.VMEM((steps * block, depth), F32),
            square,
            pltpu.VMEM((chips, columns * tall, depth), F32),
            pltpu.VMEM((total, depth), F32),
            pltpu.VMEM((total, depth), F32),
            pltpu.VMEM((total, depth), F32),
            pltpu.VMEM((steps, columns * block, depth), F32),
            pltpu.SemaphoreType.DMA((9,)),
            pltpu.SemaphoreType.DMA((columns // 2,)),
        ],
        10**9,
        middle, edge_low, edge_high, left, right, modal, kappa_cells, inverse, ending, basis,
    )[0]
    arrived = exchanged(back).reshape(steps, columns, block, depth)
    return jnp.transpose(arrived, (1, 0, 2, 3)).reshape(1, columns, size, depth)


def solution(mesh):
    return jax.shard_map(
        correction,
        mesh=mesh,
        in_specs=(
            P("tm", "tx", None, None),
            P("tm", "tx", None, None),
            P("tx", None, None),
            P("tx", None),
            P(),
            P(),
        ),
        out_specs=P("tm", "tx", None, None),
        check_vma=False,
    )
```

```python
import functools

import jax
import jax.numpy as jnp
from jax import lax
from jax.experimental import pallas as pl
from jax.experimental.pallas import tpu as pltpu
from jax.sharding import PartitionSpec as P


ALPHA = 0.05
REACH = 2
F32 = jnp.float32
BF16 = jnp.bfloat16
MIB = 2**20
VMEM_BYTES = 67043328


def split(value):
    high = value.astype(BF16)
    return high, (value - high.astype(F32)).astype(BF16)


def dot(left, right):
    return jnp.dot(left, right, preferred_element_type=F32)


def shifted(array, axis, by):
    count = lax.axis_size(axis)
    pairs = [(i, i + by) for i in range(count) if 0 <= i + by < count]
    return lax.ppermute(array, axis, pairs)


def cut(value, rows, out, base, blocks):
    size = value.shape[0]
    block = size // blocks
    tall = block + 2 * REACH
    rows[pl.ds(REACH, size), :] = value
    for target in range(blocks):
        out[target, pl.ds(base, tall), :] = rows[pl.ds(block * target, tall), :]


def fill_weights(weights, first_half, second_half):
    depth = first_half.shape[0]
    first_high, first_low = split(first_half)
    weights[:depth, :depth] = first_high
    weights[:depth, depth:] = first_low
    if second_half is None:
        weights[depth:, :depth] = first_high
        weights[depth:, depth:] = jnp.zeros_like(first_low)
    else:
        second_high, second_low = split(second_half)
        weights[depth:, :depth] = second_high
        weights[depth:, depth:] = second_low


def times_matrix(value, weights):
    depth = value.shape[1]
    wide = dot(jnp.concatenate(split(value), axis=1), weights[...])
    return wide[:, :depth] + wide[:, depth:]


def residual_kernel(
    blocks, inner, state, other, initial, force, low, high, kappa, rates, basis, out,
    here, past, pushed, parts, rows, levels, turned, weights, sides, plain_ref, rates_ref, loads, stores, extras,
):
    columns, size, depth = state.shape
    tall = size // blocks + 2 * REACH
    step_here = lax.axis_index("tm")
    odd = step_here % 2 == 1
    first = step_here == 0
    if inner:
        mine = list(range(2, columns - 2))
        wide = list(range(1, columns - 1))
    else:
        mine = [0, 1, columns - 2, columns - 1]
        wide = [0, 1, 2, columns - 3, columns - 2, columns - 1]

    def load(kind, x):
        source, target = ((state, here), (other, past), (force, pushed))[kind]
        target = target.at[x, pl.ds(8, size), :] if kind == 0 else target.at[x]
        return pltpu.make_async_copy(source.at[x], target, loads.at[kind, x])

    def level(x):
        return here[x, pl.ds(8, size), :]

    small = [(basis, plain_ref), (rates, rates_ref), (kappa, levels.at[pl.ds(0, columns), :])]
    if not inner:
        small += [(low, sides.at[0]), (high, sides.at[1])]
    small = [pltpu.make_async_copy(*ends, extras.at[i]) for i, ends in enumerate(small)]
    levels[...] = jnp.zeros_like(levels)
    for copy in small:
        copy.start()
    for x in wide:
        load(0, x).start()
        if x in mine:
            load(2, x).start()

    @pl.when(odd)
    def _():
        for x in mine:
            load(1, x).start()

    @pl.when(first)
    def _():
        for x in mine:
            pltpu.make_async_copy(initial.at[x], past.at[x], loads.at[1, x]).start()

    here[:, :8, :] = jnp.zeros((columns, 8, depth), F32)
    here[:, 8 + size :, :] = jnp.zeros((columns, 8, depth), F32)

    rows[...] = jnp.zeros_like(rows)
    for copy in small:
        copy.wait()
    plain = plain_ref[...]
    fill_weights(weights, plain, -plain * rates_ref[...])
    for part in range(size // depth):
        where = pl.ds(part * depth, depth)
        turned[where, :] = jnp.transpose(levels[:, where])

    def column(x, left, right, base, which):
        load(2, x).wait()

        @pl.when(jnp.logical_or(odd, first))
        def _():
            load(1, x).wait()

        center = level(x)
        up = here[x, pl.ds(7, size), :]
        down = here[x, pl.ds(9, size), :]
        square = center * center
        beside = left + right + up + down
        across = jnp.broadcast_to(pltpu.roll(turned[...], (depth - x) % depth, 1)[:, :1], (size, depth))
        value = (
            pushed[x]
            - center
            + jnp.where(jnp.logical_or(odd, first), past[x], 0.0)
            - across * (4.0 * center - beside)
            - 0.5 * (square * center) / (1.0 + square)
        )
        value_high, value_low = split(value)
        center_high, center_low = split(center)
        joined_high = jnp.concatenate([value_high, center_high], axis=1)
        joined_low = jnp.concatenate([value_low, center_low], axis=1)
        product = dot(joined_high, weights[...])
        modal = product[:, :depth] + product[:, depth:] + dot(joined_low, weights[:, :depth])
        cut(modal, rows.at[which], parts, base, blocks)

    def store(step):
        where = pl.ds(pl.multiple_of(step * 2 * tall, 8), 2 * tall)
        return pltpu.make_async_copy(parts.at[:, where, :], out.at[:, where, :], stores.at[step])

    if inner:
        load(0, 1).wait()
        load(0, 2).wait()

        def pair(step, carry):
            base = pl.multiple_of(step * 2 * tall, 8)
            for which in range(2):
                x = 2 + 2 * step + which
                load(0, x + 1).wait()
                column(x, level(x - 1), level(x + 1), base + which * tall, which)
            store(step).start()
            return carry

        lax.fori_loop(0, len(mine) // 2, pair, 0)
    else:
        for x in wide:
            load(0, x).wait()
        column(0, sides[0], level(1), 0, 0)
        column(1, level(0), level(2), tall, 1)
        store(0).start()
        column(columns - 2, level(columns - 3), level(columns - 1), 2 * tall, 0)
        column(columns - 1, level(columns - 2), sides[1], 3 * tall, 1)
        store(1).start()
    for step in range(len(mine) // 2):
        store(step).wait()


def modes_kernel(block, count, spans, edge, state, other, kappa, rates, basis, *rest):
    pieces = rest[:count]
    first_out, second_out, third_out, near, far, strip, gathered, weights, plain_ref, rates_ref, edges, cells, loads, stores = rest[count:]
    broad, _ = near.shape[1:]
    window = far.shape[2]
    chips = count + 1
    steps = 2 * chips
    size = block * steps
    tall = block + 2 * REACH
    room = (strip.shape[1] - broad) // 2
    here = lax.axis_index("tm")
    chip = here // 2
    odd = here % 2 == 1
    width = sum(stop - start for start, stop in spans)
    near_start = pl.multiple_of(near_begin(here, block, broad, size), 8)

    def copies(source):
        made = []
        at = 0
        for start, stop in spans:
            take = pl.ds(start, stop - start)
            put = pl.ds(at, stop - start)
            made.append((source.at[take, pl.ds(near_start, broad), :], near.at[put]))
            made += [(pieces[by].at[take], far.at[by, put]) for by in range(count)]
            at += stop - start
        return [pltpu.make_async_copy(*ends, loads.at[i]) for i, ends in enumerate(made)]

    small = [(basis, plain_ref), (rates, rates_ref), (kappa, cells)]
    if edge is not None:
        small.append((edge, edges))
    small = [pltpu.make_async_copy(*ends, stores.at[i]) for i, ends in enumerate(small)]

    @pl.when(odd)
    def _():
        for copy in copies(state):
            copy.start()

    @pl.when(jnp.logical_not(odd))
    def _():
        for copy in copies(other):
            copy.start()

    for copy in small:
        copy.start()
    strip[...] = jnp.zeros_like(strip)
    for copy in small:
        copy.wait()
    fill_weights(weights, plain_ref[...], None)
    if edge is None:
        chunk = 2 * tall

        def factors(step, carry):
            base = pl.multiple_of(step * chunk, 8)
            second_out[pl.ds(base, chunk), :], third_out[pl.ds(base, chunk), :] = time_factors(
                cells[pl.ds(base, chunk), :], rates_ref[...], steps
            )
            return carry

        lax.fori_loop(0, cells.shape[0] // chunk, factors, 0)
    for copy in copies(state):
        copy.wait()
    begin = block * here - REACH + room

    def gather(source, start, extent):
        for x in range(width):
            strip[x % 2, pl.ds(room, extent), :] = source(x)
            gathered[pl.ds(x * tall, tall), :] = strip[x % 2, pl.ds(begin - start, tall), :]
        return times_matrix(gathered[...], weights)

    first_out[chip] = gather(lambda x: near[x], near_start, broad)

    far_start = window_start(here, block, window, size)
    strip[...] = jnp.zeros_like(strip)

    def far_slot(by, carry):
        first_out[(chip - by - 1 + chips) % chips] = gather(lambda x: far[by, x], far_start, window)
        return carry

    lax.fori_loop(0, count, far_slot, 0)
    if edge is not None:
        two = REACH * tall
        for n in range(steps):
            left = edges[n, :two, :]
            right = edges[n, two:, :]
            if n and n % 2 == 0:
                left = left + first_out[n // 2 - 1, :two, :]
                right = right + first_out[n // 2 - 1, two:, :]
            second_out[n] = left
            third_out[n] = right
        second_out[steps] = cells[:two, :]
        third_out[steps] = cells[cells.shape[0] - two :, :]


def time_factors(kappa, rates, steps):
    inverse = 1.0 / (1.0 + rates + 4.0 * kappa)
    power = inverse
    for _ in range(steps - 1):
        power = power * inverse
    return inverse, ALPHA / (1.0 - ALPHA * power)


def rim_kernel(block, count, spans, edge, state, other, kappa, rates, basis, *rest):
    outs, scratch = rest[count : count + 2], rest[count + 2 :]
    modes_kernel(block, count, spans, edge, state, other, kappa, rates, basis, *rest[:count], scratch[0], *outs, *scratch[1:])


def fill_kernel(block, count, spans, state, other, edge_low, edge_high, kappa, rates, basis, *rest):
    bundle, scratch = rest[count], rest[count + 1 :]
    modal, inverse, ending, ends, turned, sems = scratch[:6]
    steps = edge_low.shape[0] - 1
    sides = [pltpu.make_async_copy(edge, ends.at[i], sems.at[i]) for i, edge in enumerate((edge_low, edge_high))]
    for copy in sides:
        copy.start()
    inner = scratch[6:]
    modes_kernel(block, count, spans, None, state, other, kappa, rates, basis, *rest[:count], modal, inverse, ending, *inner)
    plain_ref, rates_ref, cells = inner[5], inner[6], inner[8]
    turned[pl.ds(0, plain_ref.shape[0]), :] = jnp.transpose(plain_ref[...])
    turned[pl.ds(plain_ref.shape[0], 8), :] = jnp.broadcast_to(rates_ref[...], (8, plain_ref.shape[1]))
    for copy in sides:
        copy.wait()
    copies = [
        pltpu.make_async_copy(source, bundle.at[pl.ds(start, source.shape[0]), :], sems.at[2 + i])
        for i, (source, start) in enumerate(bundle_parts(modal, cells, inverse, ending, ends, turned, steps))
    ]
    for copy in copies:
        copy.start()
    for copy in copies:
        copy.wait()


def bundle_parts(modal, cells, inverse, ending, ends, turned, steps):
    parts = [modal.at[m] for m in range(steps // 2 - 1)] + [cells, inverse, ending]
    parts += [ends.at[side, n] for side in range(2) for n in range(steps)] + [turned]
    placed = []
    at = 0
    for part in parts:
        placed.append((part, at))
        at += part.shape[0]
    return placed


def relax_kernel(
    block, middle, left, right, bundle, out,
    known, source, older, newer, gathered, weights, modal, kappa, inverse, ending, ends, turned, loads,
):
    steps, inner, depth = middle.shape
    tall = block + 2 * REACH
    chunk = REACH * tall
    columns = inner // tall + 2 * REACH
    total = inner + 4 * chunk
    pad = older.shape[1] - total
    front = pad // 2
    own = pl.ds(chunk, total - 2 * chunk)
    parts = bundle_parts(modal, kappa.at[own, :], inverse.at[own, :], ending.at[own, :], ends, turned, steps)
    copies = [
        pltpu.make_async_copy(bundle.at[pl.ds(start, target.shape[0]), :], target, loads.at[i])
        for i, (target, start) in enumerate(parts)
    ]
    for copy in copies:
        copy.start()
    older[:, :front, :] = jnp.zeros((steps, front, depth), F32)
    older[:, front + total :, :] = jnp.zeros((steps, pad - front, depth), F32)
    for ghost, base in ((left, 0), (right, total - chunk)):
        kappa[pl.ds(base, chunk), :] = ghost[steps]
    copies[-1].wait()
    fill_weights(weights, turned[:depth, :], None)
    for base in (0, total - chunk):
        at = pl.ds(base, chunk)
        inverse[at, :], ending[at, :] = time_factors(kappa[at, :], turned[depth : depth + 1, :], steps)

    def solve(values, inv, end):
        last = values(0) * inv
        for n in range(1, steps):
            last = (values(n) + last) * inv
        return end * last

    def first(value, base):
        inv = inverse[pl.ds(base, chunk), :]
        run = solve(value, inv, ending[pl.ds(base, chunk), :])
        for n in range(steps):
            run = (known[n, pl.ds(base, chunk), :] + run) * inv
            older[n, pl.ds(base + front, chunk), :] = run

    def keep(value, base):
        def kept(n):
            made = value(n)
            known[n, pl.ds(base, chunk), :] = made
            return made

        return kept

    first(keep(lambda n: left[n], 0), 0)
    first(keep(lambda n: right[n], total - chunk), total - chunk)
    for copy in copies[:-1]:
        copy.wait()
    first(keep(lambda n: ends[0, n], chunk), chunk)
    first(keep(lambda n: ends[1, n], total - 2 * chunk), total - 2 * chunk)

    def first_middle(step, carry):
        at = pl.multiple_of(step * chunk, 8)
        base = pl.multiple_of(at + 2 * chunk, 8)

        def value(n):
            made = middle[n, pl.ds(at, chunk), :]
            if n and n % 2 == 0:
                made = made + modal[n // 2 - 1, pl.ds(at, chunk), :]
            return made

        first(keep(value, base), base)
        return carry

    lax.fori_loop(0, inner // chunk, first_middle, 0)

    def term(field, base, size, n):
        beside = (
            field[n, pl.ds(base + front - 1, size), :]
            + field[n, pl.ds(base + front + 1, size), :]
            + field[n, pl.ds(base + front - tall, size), :]
            + field[n, pl.ds(base + front + tall, size), :]
        )
        return known[n, pl.ds(base, size), :] + kappa[pl.ds(base, size), :] * beside

    def second(step, carry):
        base = pl.multiple_of(step * chunk, 8) + tall
        inv = inverse[pl.ds(base, chunk), :]

        def value(n):
            made = term(older, base, chunk, n)
            source[n, :chunk, :] = made
            return made

        run = solve(value, inv, ending[pl.ds(base, chunk), :])
        for n in range(steps):
            run = (source[n, :chunk, :] + run) * inv
            newer[n, pl.ds(base + front, chunk), :] = run
        return carry

    lax.fori_loop(0, (columns + 2) // 2, second, 0)

    def third(base):
        inv = inverse[pl.ds(base, block), :]

        def value(n):
            made = term(newer, base, block, n)
            source[n, :block, :] = made
            return made

        run = solve(value, inv, ending[pl.ds(base, block), :])
        for n in range(steps):
            run = (source[n, :block, :] + run) * inv
            gathered[pl.ds(n * block, block), :] = run
        gathered[...] = times_matrix(gathered[...], weights)

    def third_pair(step, carry):
        at = pl.multiple_of(step * 2 * tall, 8)
        to = pl.multiple_of(step * 2 * block, 8)
        for which in range(2):
            third(at + chunk + which * tall + REACH)
            for n in range(steps):
                out[n, pl.ds(to + which * block, block), :] = gathered[pl.ds(n * block, block), :]
        return carry

    lax.fori_loop(0, columns // 2, third_pair, 0)


SPACES = {"v": pltpu.VMEM, "h": pltpu.HBM}


def call(kernel, outs, spaces, scratch, flops, *operands, limit=None):
    shapes = [jax.ShapeDtypeStruct(shape, F32) for shape, _ in outs]
    return pl.pallas_call(
        kernel,
        out_shape=shapes,
        in_specs=[pl.BlockSpec(memory_space=SPACES[space]) for space in spaces],
        out_specs=[pl.BlockSpec(memory_space=SPACES[space]) for _, space in outs],
        scratch_shapes=scratch,
        cost_estimate=pl.CostEstimate(flops=flops, bytes_accessed=10**6, transcendentals=0),
        compiler_params=pltpu.CompilerParams(vmem_limit_bytes=60 * MIB if limit is None else limit),
    )(*operands)


def paired(array):
    count = lax.axis_size("tm")
    return lax.ppermute(array, "tm", [(i, i ^ 1) for i in range(count)])


def exchanged(array):
    return lax.all_to_all(array, "tm", split_axis=0, concat_axis=0, tiled=True)


def near_begin(device, block, broad, size):
    return jnp.clip((block * device - REACH) // 8 * 8, 0, size - broad)


def window_start(device, block, window, size):
    return jnp.clip(block * device - 4, 0, size - window)


def spread(mine, other, here, block, window, by):
    count = lax.axis_size("tm")
    start = window_start((here + 2 * by) % count, block, window, mine.shape[1])
    rows = jnp.where(
        here % 2 == 1,
        lax.dynamic_slice_in_dim(mine, start, window, 1),
        lax.dynamic_slice_in_dim(other, start, window, 1),
    )
    return lax.ppermute(rows, "tm", [(i, (i + 2 * by) % count) for i in range(count - 2)])


def correction(state, force, u_init, kappa, rates, basis):
    steps = lax.axis_size("tm")
    here = lax.axis_index("tm")
    chips = steps // 2
    columns, size, depth = u_init.shape
    block = size // steps
    tall = block + 2 * REACH
    chunk = REACH * tall
    window = block + 8
    broad = (block + 23) // 8 * 8
    inside = columns - 2 * REACH
    total = columns * tall + 2 * chunk
    front = (tall + 15) // 8 * 8
    square = pltpu.VMEM((2 * depth, 2 * depth), BF16)
    constants = [pltpu.VMEM((depth, depth), F32), pltpu.VMEM((1, depth), F32)]
    mine = state[0]
    other = paired(mine)
    low = shifted(mine[-1], "tx", 1)
    high = shifted(mine[0], "tx", -1)
    rates_row = rates.reshape(1, depth)
    pieces = []
    for by in range(1, chips):
        pieces.append(spread(mine, other, here, block, window, by))

    def residual(inner, count, flops):
        return call(
            functools.partial(residual_kernel, steps, inner),
            [((steps, count * tall, depth), "h")],
            "hhhhhhhhh",
            [
                pltpu.VMEM((columns, size + 16, depth), F32),
                pltpu.VMEM(u_init.shape, F32),
                pltpu.VMEM(u_init.shape, F32),
                pltpu.VMEM((steps, count * tall, depth), F32),
                pltpu.VMEM((2, size + 8, depth), F32),
                pltpu.VMEM((depth, size), F32),
                pltpu.VMEM((size, depth), F32),
                square,
                pltpu.VMEM((2, size, depth), F32),
                *constants,
                pltpu.SemaphoreType.DMA((3, columns)),
                pltpu.SemaphoreType.DMA((count // 2,)),
                pltpu.SemaphoreType.DMA((5,)),
            ],
            flops,
            mine, other, u_init, force[0], low, high, kappa, rates_row, basis,
        )[0]

    edge = residual(False, 2 * REACH, 2 * 10**9)
    edge = exchanged(edge)
    middle = residual(True, columns - 2 * REACH, 6 * 10**9)
    middle = exchanged(middle)
    kappa_wide = jnp.pad(kappa, ((0, 0), (REACH, REACH)))
    kappa_mine = lax.dynamic_slice_in_dim(kappa_wide, here * block, tall, 1)
    kappa_cells = jnp.broadcast_to(kappa_mine[:, :, None], kappa_mine.shape + (depth,)).reshape(-1, depth)

    def modes_scratch(width):
        return [
            pltpu.VMEM((width, broad, depth), F32),
            pltpu.VMEM((chips - 1, width, window, depth), F32),
            pltpu.VMEM((2, broad + 32, depth), F32),
            pltpu.VMEM((width * tall, depth), F32),
            square,
            *constants,
            pltpu.VMEM((steps, 2 * chunk, depth), F32),
            pltpu.VMEM((columns * tall, depth), F32),
            pltpu.SemaphoreType.DMA((2 * chips,)),
            pltpu.SemaphoreType.DMA((4,)),
        ]

    edge_low, edge_high = call(
        functools.partial(rim_kernel, block, chips - 1, [(0, REACH), (columns - REACH, columns)]),
        [((steps + 1, chunk, depth), "v")] * 2,
        "h" * (5 + chips),
        [pltpu.VMEM((chips, 2 * chunk, depth), F32)] + modes_scratch(2 * REACH),
        10**9,
        edge, mine, other, kappa_cells, rates_row, basis, *pieces,
    )
    left = shifted(edge_high, "tx", 1)
    right = shifted(edge_low, "tx", -1)
    far = [
        pltpu.VMEM((chips, inside * tall, depth), F32),
        pltpu.VMEM((columns * tall, depth), F32),
        pltpu.VMEM((columns * tall, depth), F32),
        pltpu.VMEM((2, steps + 1, chunk, depth), F32),
        pltpu.VMEM((depth + 8, depth), F32),
    ]
    rows = (chips - 1) * inside * tall + 3 * columns * tall + 2 * steps * chunk + depth + 8
    room = 16 * (middle.size + 2 * left.size + u_init.size)
    rows = max(rows, -(-(room + MIB) // (4096 * depth)) * 1024)
    bundle = call(
        functools.partial(fill_kernel, block, chips - 1, [(REACH, columns - REACH)]),
        [((rows, depth), "h")],
        "h" * (6 + chips),
        far + [pltpu.SemaphoreType.DMA((2 * steps + chips + 8,))] + modes_scratch(inside),
        10**9,
        mine, other, edge_low, edge_high, kappa_cells, rates_row, basis, *pieces,
    )[0]
    wide = pltpu.VMEM((total, depth), F32)
    back = call(
        functools.partial(relax_kernel, block),
        [((steps, columns * block, depth), "v")],
        "vvvh",
        [
            pltpu.VMEM((steps, total, depth), F32),
            pltpu.VMEM((steps, chunk, depth), F32),
            pltpu.VMEM((steps, total + 2 * front, depth), F32),
            pltpu.VMEM((steps, total + 2 * front, depth), F32),
            pltpu.VMEM((steps * block, depth), F32),
            square,
            far[0],
            wide,
            wide,
            wide,
            *far[3:],
            pltpu.SemaphoreType.DMA((2 * steps + chips + 3,)),
        ],
        10**9,
        middle, left, right, bundle,
        limit=VMEM_BYTES - room,
    )[0]
    arrived = exchanged(back).reshape(steps, columns, block, depth)
    return jnp.transpose(arrived, (1, 0, 2, 3)).reshape(1, columns, size, depth)


def solution(mesh):
    return jax.shard_map(
        correction,
        mesh=mesh,
        in_specs=(
            P("tm", "tx", None, None),
            P("tm", "tx", None, None),
            P("tx", None, None),
            P("tx", None),
            P(),
            P(),
        ),
        out_specs=P("tm", "tx", None, None),
        check_vma=False,
    )
```

```python
import functools

import jax
import jax.numpy as jnp
from jax import lax
from jax.experimental import pallas as pl
from jax.experimental.pallas import tpu as pltpu
from jax.sharding import PartitionSpec as P


ALPHA = 0.05
REACH = 2
F32 = jnp.float32
BF16 = jnp.bfloat16
MIB = 2**20
VMEM_BYTES = 67043328


def split(value):
    high = value.astype(BF16)
    return high, (value - high.astype(F32)).astype(BF16)


def dot(left, right):
    return jnp.dot(left, right, preferred_element_type=F32)


def shifted(array, axis, by):
    count = lax.axis_size(axis)
    pairs = [(i, i + by) for i in range(count) if 0 <= i + by < count]
    return lax.ppermute(array, axis, pairs)


def cut(value, rows, out, base, blocks):
    size = value.shape[0]
    block = size // blocks
    tall = block + 2 * REACH
    rows[pl.ds(REACH, size), :] = value
    for target in range(blocks):
        out[target, pl.ds(base, tall), :] = rows[pl.ds(block * target, tall), :]


def fill_weights(weights, first_half, second_half):
    depth = first_half.shape[0]
    first_high, first_low = split(first_half)
    weights[:depth, :depth] = first_high
    weights[:depth, depth:] = first_low
    if second_half is None:
        weights[depth:, :depth] = first_high
        weights[depth:, depth:] = jnp.zeros_like(first_low)
    else:
        second_high, second_low = split(second_half)
        weights[depth:, :depth] = second_high
        weights[depth:, depth:] = second_low


def times_matrix(value, weights):
    depth = value.shape[1]
    wide = dot(jnp.concatenate(split(value), axis=1), weights[...])
    return wide[:, :depth] + wide[:, depth:]


def residual_kernel(
    blocks, inner, state, other, initial, force, low, high, kappa, rates, basis, out,
    here, past, pushed, parts, rows, levels, turned, weights, sides, plain_ref, rates_ref, loads, stores, extras,
):
    columns, size, depth = state.shape
    tall = size // blocks + 2 * REACH
    step_here = lax.axis_index("tm")
    odd = step_here % 2 == 1
    first = step_here == 0
    if inner:
        group = 4 if (columns - 4) % 4 == 0 else 2
        count = (columns - 4) // group
        spans = [(2 + group * step, group) for step in range(count)]
        wide = [(1 if step == 0 else start + 1, group + 2 if step == 0 else group) for step, (start, _) in enumerate(spans)]
    else:
        group = 2
        count = 2
        spans = [(0, 2), (columns - 2, 2)]
        wide = [(0, 3), (columns - 3, 3)]

    def load(kind, step, source=None):
        start, extent = (wide if kind == 0 else spans)[step]
        take = pl.ds(start, extent)
        source = (state, other, force)[kind] if source is None else source
        target = here.at[take, pl.ds(8, size), :] if kind == 0 else (past, pushed)[kind - 1].at[take]
        return pltpu.make_async_copy(source.at[take], target, loads.at[kind, step])

    def arrive(step):
        start = pl.ds(0, group)
        pltpu.make_async_copy(force.at[start], pushed.at[start], loads.at[2, step]).wait()
        if inner:
            pltpu.make_async_copy(state.at[start], here.at[start, pl.ds(8, size), :], loads.at[0, step]).wait()

        @pl.when(jnp.logical_or(odd, first))
        def _():
            pltpu.make_async_copy(other.at[start], past.at[start], loads.at[1, step]).wait()

    def level(x):
        return here[x, pl.ds(8, size), :]

    small = [(basis, plain_ref), (rates, rates_ref), (kappa, levels.at[pl.ds(0, columns), :])]
    if not inner:
        small += [(low, sides.at[0]), (high, sides.at[1])]
    small = [pltpu.make_async_copy(*ends, extras.at[i]) for i, ends in enumerate(small)]
    levels[...] = jnp.zeros_like(levels)
    for copy in small:
        copy.start()
    for step in range(count):
        load(0, step).start()
        load(2, step).start()

    @pl.when(odd)
    def _():
        for step in range(count):
            load(1, step).start()

    @pl.when(first)
    def _():
        for step in range(count):
            load(1, step, initial).start()

    here[:, :8, :] = jnp.zeros((columns, 8, depth), F32)
    here[:, 8 + size :, :] = jnp.zeros((columns, 8, depth), F32)

    rows[...] = jnp.zeros_like(rows)
    for copy in small:
        copy.wait()
    plain = plain_ref[...]
    fill_weights(weights, plain, -plain * rates_ref[...])
    for part in range(size // depth):
        where = pl.ds(part * depth, depth)
        turned[where, :] = jnp.transpose(levels[:, where])

    def residual(x, left, right, across):
        center = level(x)
        square = center * center
        beside = left + right + here[x, pl.ds(7, size), :] + here[x, pl.ds(9, size), :]
        return (
            pushed[x]
            - center
            + jnp.where(jnp.logical_or(odd, first), past[x], 0.0)
            - across * (4.0 * center - beside)
            - 0.5 * (square * center) / (1.0 + square)
        )

    def columns_of(x, group, sides_of, base):
        rolled = turned[...] if isinstance(x, int) else pltpu.roll(turned[...], depth - x, 1)
        at = x if isinstance(x, int) else 0
        for begin in range(0, group, 2):
            highs, lows = [], []
            for which in range(begin, begin + 2):
                across = jnp.broadcast_to(rolled[:, at + which : at + which + 1], (size, depth))
                value_high, value_low = split(residual(x + which, *sides_of(x + which), across))
                center_high, center_low = split(level(x + which))
                highs.append(jnp.concatenate([value_high, center_high], axis=1))
                lows.append(jnp.concatenate([value_low, center_low], axis=1))
            product = dot(jnp.concatenate(highs, axis=0), weights[...])
            modal = product[:, :depth] + product[:, depth:] + dot(jnp.concatenate(lows, axis=0), weights[:, :depth])
            for which in range(2):
                part = modal[which * size : (which + 1) * size]
                cut(part, rows.at[begin + which], parts, base + (begin + which) * tall, blocks)

    def store(step):
        where = pl.ds(pl.multiple_of(step * group * tall, 8), group * tall)
        return pltpu.make_async_copy(parts.at[:, where, :], out.at[:, where, :], stores.at[step])

    if inner:
        pair_of = pl.ds(0, 2)
        pltpu.make_async_copy(state.at[pair_of], here.at[pair_of, pl.ds(8, size), :], loads.at[0, 0]).wait()

        def pair(step, carry):
            base = pl.multiple_of(step * group * tall, 8)
            x = 2 + group * step
            arrive(step)
            columns_of(x, group, lambda at: (level(at - 1), level(at + 1)), base)
            store(step).start()
            return carry

        lax.fori_loop(0, count, pair, 0)
    else:
        for step in range(count):
            load(0, step).wait()
            arrive(step)
        columns_of(0, 2, lambda at: (sides[0] if at == 0 else level(0), level(at + 1)), 0)
        store(0).start()
        last = columns - 1
        columns_of(last - 1, 2, lambda at: (level(at - 1), sides[1] if at == last else level(last)), 2 * tall)
        store(1).start()
    for step in range(count):
        store(step).wait()


def modes_kernel(block, count, spans, edge, state, other, kappa, rates, basis, *rest):
    pieces = rest[:count]
    first_out, second_out, third_out, near, far, strip, gathered, weights, plain_ref, rates_ref, edges, cells, loads, stores = rest[count:]
    broad, _ = near.shape[1:]
    window = far.shape[2]
    chips = count + 1
    steps = 2 * chips
    size = block * steps
    tall = block + 2 * REACH
    room = (strip.shape[1] - broad) // 2
    here = lax.axis_index("tm")
    chip = here // 2
    odd = here % 2 == 1
    width = sum(stop - start for start, stop in spans)
    near_start = pl.multiple_of(near_begin(here, block, broad, size), 8)

    def copies(source):
        made = []
        at = 0
        for start, stop in spans:
            take = pl.ds(start, stop - start)
            put = pl.ds(at, stop - start)
            made.append((source.at[take, pl.ds(near_start, broad), :], near.at[put]))
            made += [(pieces[by].at[take], far.at[by, put]) for by in range(count)]
            at += stop - start
        return [pltpu.make_async_copy(*ends, loads.at[i]) for i, ends in enumerate(made)]

    small = [(basis, plain_ref), (rates, rates_ref), (kappa, cells)]
    if edge is not None:
        small.append((edge, edges))
    small = [pltpu.make_async_copy(*ends, stores.at[i]) for i, ends in enumerate(small)]

    @pl.when(odd)
    def _():
        for copy in copies(state):
            copy.start()

    @pl.when(jnp.logical_not(odd))
    def _():
        for copy in copies(other):
            copy.start()

    for copy in small:
        copy.start()
    strip[...] = jnp.zeros_like(strip)
    for copy in small:
        copy.wait()
    fill_weights(weights, plain_ref[...], None)
    if edge is None:
        chunk = 2 * tall

        def factors(step, carry):
            base = pl.multiple_of(step * chunk, 8)
            second_out[pl.ds(base, chunk), :], third_out[pl.ds(base, chunk), :] = time_factors(
                cells[pl.ds(base, chunk), :], rates_ref[...], steps
            )
            return carry

        lax.fori_loop(0, cells.shape[0] // chunk, factors, 0)
    for copy in copies(state):
        copy.wait()
    begin = block * here - REACH + room

    def keep(slot, value):
        first_out[pl.ds(pl.multiple_of(slot * (width * tall), 8), width * tall), :] = value

    def gather(source, start, extent):
        for x in range(width):
            strip[x % 2, pl.ds(room, extent), :] = source(x)
            gathered[pl.ds(x * tall, tall), :] = strip[x % 2, pl.ds(begin - start, tall), :]
        return times_matrix(gathered[...], weights)

    keep(chip, gather(lambda x: near[x], near_start, broad))

    far_start = window_start(here, block, window, size)
    strip[...] = jnp.zeros_like(strip)

    def far_slot(by, carry):
        keep((chip - by - 1 + chips) % chips, gather(lambda x: far[by, x], far_start, window))
        return carry

    lax.fori_loop(0, count, far_slot, 0)
    if edge is not None:
        two = REACH * tall
        for n in range(steps):
            left = edges[n, :two, :]
            right = edges[n, two:, :]
            if n and n % 2 == 0:
                at = (n // 2 - 1) * 2 * two
                left = left + first_out[at : at + two, :]
                right = right + first_out[at + two : at + 2 * two, :]
            second_out[n * two : (n + 1) * two, :] = left
            third_out[n * two : (n + 1) * two, :] = right
        second_out[steps * two :, :] = cells[:two, :]
        third_out[steps * two :, :] = cells[cells.shape[0] - two :, :]


def time_factors(kappa, rates, steps):
    inverse = 1.0 / (1.0 + rates + 4.0 * kappa)
    power = inverse
    for _ in range(steps - 1):
        power = power * inverse
    return inverse, ALPHA / (1.0 - ALPHA * power)


def rim_kernel(block, count, spans, edge, state, other, kappa, rates, basis, *rest):
    outs, scratch = rest[count : count + 2], rest[count + 2 :]
    modes_kernel(block, count, spans, edge, state, other, kappa, rates, basis, *rest[:count], scratch[0], *outs, *scratch[1:])


def fill_kernel(block, count, spans, state, other, edge_low, edge_high, kappa, rates, basis, *rest):
    bundle, scratch = rest[count], rest[count + 1 :]
    modal, inverse, ending, ends, turned, sems = scratch[:6]
    sides = [pltpu.make_async_copy(edge, ends.at[i], sems.at[i]) for i, edge in enumerate((edge_low, edge_high))]
    for copy in sides:
        copy.start()
    inner = scratch[6:]
    modes_kernel(block, count, spans, None, state, other, kappa, rates, basis, *rest[:count], modal, inverse, ending, *inner)
    plain_ref, rates_ref, cells = inner[5], inner[6], inner[8]
    turned[pl.ds(0, plain_ref.shape[0]), :] = jnp.transpose(plain_ref[...])
    turned[pl.ds(plain_ref.shape[0], 8), :] = jnp.broadcast_to(rates_ref[...], (8, plain_ref.shape[1]))
    for copy in sides:
        copy.wait()
    copies = [
        pltpu.make_async_copy(source, bundle.at[pl.ds(start, source.shape[0]), :], sems.at[2 + i])
        for i, (source, start) in enumerate(bundle_parts(modal, cells, inverse, ending, ends, turned))
    ]
    for copy in copies:
        copy.start()
    for copy in copies:
        copy.wait()


def bundle_parts(modal, cells, inverse, ending, ends, turned):
    placed = []
    at = 0
    for part in (cells, inverse, ending, ends.at[0], ends.at[1], turned, modal):
        placed.append((part, at))
        at += part.shape[0]
    return placed


def relax_kernel(
    block, middle, left, right, bundle, out,
    known, source, older, newer, gathered, weights, modal, kappa, inverse, ending, ends, turned, loads,
):
    steps, inner, depth = middle.shape
    tall = block + 2 * REACH
    chunk = REACH * tall
    columns = inner // tall + 2 * REACH
    total = inner + 4 * chunk
    pad = older.shape[1] - total
    front = pad // 2
    own = pl.ds(chunk, total - 2 * chunk)
    parts = bundle_parts(modal, kappa.at[own, :], inverse.at[own, :], ending.at[own, :], ends, turned)
    copies = [
        pltpu.make_async_copy(bundle.at[pl.ds(start, target.shape[0]), :], target, loads.at[i])
        for i, (target, start) in enumerate(parts)
    ]
    for copy in copies:
        copy.start()
    older[:, :front, :] = jnp.zeros((steps, front, depth), F32)
    older[:, front + total :, :] = jnp.zeros((steps, pad - front, depth), F32)
    for ghost, base in ((left, 0), (right, total - chunk)):
        kappa[pl.ds(base, chunk), :] = ghost[steps * chunk :, :]
    copies[5].wait()
    fill_weights(weights, turned[:depth, :], None)
    for base in (0, total - chunk):
        at = pl.ds(base, chunk)
        inverse[at, :], ending[at, :] = time_factors(kappa[at, :], turned[depth : depth + 1, :], steps)

    def solve(values, inv, end):
        last = values(0) * inv
        for n in range(1, steps):
            last = (values(n) + last) * inv
        return end * last

    def first(value, base):
        inv = inverse[pl.ds(base, chunk), :]
        run = solve(value, inv, ending[pl.ds(base, chunk), :])
        for n in range(steps):
            run = (known[n, pl.ds(base, chunk), :] + run) * inv
            older[n, pl.ds(base + front, chunk), :] = run

    def keep(value, base):
        def kept(n):
            made = value(n)
            known[n, pl.ds(base, chunk), :] = made
            return made

        return kept

    first(keep(lambda n: left[n * chunk : (n + 1) * chunk, :], 0), 0)
    first(keep(lambda n: right[n * chunk : (n + 1) * chunk, :], total - chunk), total - chunk)
    for copy in copies[:5]:
        copy.wait()
    first(keep(lambda n: ends[0, n * chunk : (n + 1) * chunk, :], chunk), chunk)
    first(keep(lambda n: ends[1, n * chunk : (n + 1) * chunk, :], total - 2 * chunk), total - 2 * chunk)
    copies[6].wait()

    def first_middle(step, carry):
        at = pl.multiple_of(step * chunk, 8)
        base = pl.multiple_of(at + 2 * chunk, 8)

        def value(n):
            made = middle[n, pl.ds(at, chunk), :]
            if n and n % 2 == 0:
                made = made + modal[pl.ds((n // 2 - 1) * inner + at, chunk), :]
            return made

        first(keep(value, base), base)
        return carry

    lax.fori_loop(0, inner // chunk, first_middle, 0)

    def term(field, base, size, n):
        beside = (
            field[n, pl.ds(base + front - 1, size), :]
            + field[n, pl.ds(base + front + 1, size), :]
            + field[n, pl.ds(base + front - tall, size), :]
            + field[n, pl.ds(base + front + tall, size), :]
        )
        return known[n, pl.ds(base, size), :] + kappa[pl.ds(base, size), :] * beside

    def second(step, carry):
        base = pl.multiple_of(step * chunk, 8) + tall
        inv = inverse[pl.ds(base, chunk), :]

        def value(n):
            made = term(older, base, chunk, n)
            source[n, :chunk, :] = made
            return made

        run = solve(value, inv, ending[pl.ds(base, chunk), :])
        for n in range(steps):
            run = (source[n, :chunk, :] + run) * inv
            newer[n, pl.ds(base + front, chunk), :] = run
        return carry

    lax.fori_loop(0, (columns + 2) // 2, second, 0)

    def third(base):
        inv = inverse[pl.ds(base, block), :]

        def value(n):
            made = term(newer, base, block, n)
            source[n, :block, :] = made
            return made

        run = solve(value, inv, ending[pl.ds(base, block), :])
        for n in range(steps):
            run = (source[n, :block, :] + run) * inv
            gathered[pl.ds(n * block, block), :] = run
        gathered[...] = times_matrix(gathered[...], weights)

    def third_pair(step, carry):
        at = pl.multiple_of(step * 2 * tall, 8)
        to = pl.multiple_of(step * 2 * block, 8)
        for which in range(2):
            third(at + chunk + which * tall + REACH)
            for n in range(steps):
                out[n, pl.ds(to + which * block, block), :] = gathered[pl.ds(n * block, block), :]
        return carry

    lax.fori_loop(0, columns // 2, third_pair, 0)


SPACES = {"v": pltpu.VMEM, "h": pltpu.HBM}


def call(kernel, outs, spaces, scratch, flops, *operands, limit=None):
    shapes = [jax.ShapeDtypeStruct(shape, F32) for shape, _ in outs]
    return pl.pallas_call(
        kernel,
        out_shape=shapes,
        in_specs=[pl.BlockSpec(memory_space=SPACES[space]) for space in spaces],
        out_specs=[pl.BlockSpec(memory_space=SPACES[space]) for _, space in outs],
        scratch_shapes=scratch,
        cost_estimate=pl.CostEstimate(flops=flops, bytes_accessed=10**6, transcendentals=0),
        compiler_params=pltpu.CompilerParams(vmem_limit_bytes=60 * MIB if limit is None else limit),
    )(*operands)


def paired(array):
    count = lax.axis_size("tm")
    return lax.ppermute(array, "tm", [(i, i ^ 1) for i in range(count)])


def exchanged(array):
    return lax.all_to_all(array, "tm", split_axis=0, concat_axis=0, tiled=True)


def near_begin(device, block, broad, size):
    return jnp.clip((block * device - REACH) // 8 * 8, 0, size - broad)


def window_start(device, block, window, size):
    return jnp.clip(block * device - 4, 0, size - window)


def spread(mine, other, here, block, window, by):
    count = lax.axis_size("tm")
    start = window_start((here + 2 * by) % count, block, window, mine.shape[1])
    rows = jnp.where(
        here % 2 == 1,
        lax.dynamic_slice_in_dim(mine, start, window, 1),
        lax.dynamic_slice_in_dim(other, start, window, 1),
    )
    return lax.ppermute(rows, "tm", [(i, (i + 2 * by) % count) for i in range(count - 2)])


def correction(state, force, u_init, kappa, rates, basis):
    steps = lax.axis_size("tm")
    here = lax.axis_index("tm")
    chips = steps // 2
    columns, size, depth = u_init.shape
    block = size // steps
    tall = block + 2 * REACH
    chunk = REACH * tall
    window = block + 8
    broad = (block + 23) // 8 * 8
    inside = columns - 2 * REACH
    total = columns * tall + 2 * chunk
    front = (tall + 15) // 8 * 8
    square = pltpu.VMEM((2 * depth, 2 * depth), BF16)
    constants = [pltpu.VMEM((depth, depth), F32), pltpu.VMEM((1, depth), F32)]
    mine = state[0]
    other = paired(mine)
    low = shifted(mine[-1], "tx", 1)
    high = shifted(mine[0], "tx", -1)
    rates_row = rates.reshape(1, depth)
    pieces = []
    for by in range(1, chips):
        pieces.append(spread(mine, other, here, block, window, by))

    def residual(inner, count, flops):
        return call(
            functools.partial(residual_kernel, steps, inner),
            [((steps, count * tall, depth), "h")],
            "hhhhhhhhh",
            [
                pltpu.VMEM((columns, size + 16, depth), F32),
                pltpu.VMEM(u_init.shape, F32),
                pltpu.VMEM(u_init.shape, F32),
                pltpu.VMEM((steps, count * tall, depth), F32),
                pltpu.VMEM((4, size + 8, depth), F32),
                pltpu.VMEM((depth, size), F32),
                pltpu.VMEM((size, depth), F32),
                square,
                pltpu.VMEM((2, size, depth), F32),
                *constants,
                pltpu.SemaphoreType.DMA((3, max(count // 4, 2) if count % 4 == 0 else count // 2)),
                pltpu.SemaphoreType.DMA((max(count // 4, 2) if count % 4 == 0 else count // 2,)),
                pltpu.SemaphoreType.DMA((3 if inner else 5,)),
            ],
            flops,
            mine, other, u_init, force[0], low, high, kappa, rates_row, basis,
        )[0]

    edge = residual(False, 2 * REACH, 2 * 10**9)
    edge = exchanged(edge)
    middle = residual(True, columns - 2 * REACH, 6 * 10**9)
    middle = exchanged(middle)
    kappa_wide = jnp.pad(kappa, ((0, 0), (REACH, REACH)))
    kappa_mine = lax.dynamic_slice_in_dim(kappa_wide, here * block, tall, 1)
    kappa_cells = jnp.broadcast_to(kappa_mine[:, :, None], kappa_mine.shape + (depth,)).reshape(-1, depth)

    def modes_scratch(width):
        return [
            pltpu.VMEM((width, broad, depth), F32),
            pltpu.VMEM((chips - 1, width, window, depth), F32),
            pltpu.VMEM((2, broad + 32, depth), F32),
            pltpu.VMEM((width * tall, depth), F32),
            square,
            *constants,
            pltpu.VMEM((steps, 2 * chunk, depth), F32),
            pltpu.VMEM((columns * tall, depth), F32),
            pltpu.SemaphoreType.DMA((2 * chips,)),
            pltpu.SemaphoreType.DMA((4,)),
        ]

    edge_low, edge_high = call(
        functools.partial(rim_kernel, block, chips - 1, [(0, REACH), (columns - REACH, columns)]),
        [(((steps + 1) * chunk, depth), "v")] * 2,
        "h" * (5 + chips),
        [pltpu.VMEM((chips * 2 * chunk, depth), F32)] + modes_scratch(2 * REACH),
        10**9,
        edge, mine, other, kappa_cells, rates_row, basis, *pieces,
    )
    left = shifted(edge_high, "tx", 1)
    right = shifted(edge_low, "tx", -1)
    far = [
        pltpu.VMEM((chips * inside * tall, depth), F32),
        pltpu.VMEM((columns * tall, depth), F32),
        pltpu.VMEM((columns * tall, depth), F32),
        pltpu.VMEM((2, (steps + 1) * chunk, depth), F32),
        pltpu.VMEM((depth + 8, depth), F32),
    ]
    rows = chips * inside * tall + 3 * columns * tall + 2 * (steps + 1) * chunk + depth + 8
    room = 16 * (middle.size + 2 * left.size + u_init.size)
    rows = max(rows, -(-(room + MIB) // (4096 * depth)) * 1024)
    bundle = call(
        functools.partial(fill_kernel, block, chips - 1, [(REACH, columns - REACH)]),
        [((rows, depth), "h")],
        "h" * (6 + chips),
        far + [pltpu.SemaphoreType.DMA((9,))] + modes_scratch(inside),
        10**9,
        mine, other, edge_low, edge_high, kappa_cells, rates_row, basis, *pieces,
    )[0]
    wide = pltpu.VMEM((total, depth), F32)
    back = call(
        functools.partial(relax_kernel, block),
        [((steps, columns * block, depth), "v")],
        "vvvh",
        [
            pltpu.VMEM((steps, total, depth), F32),
            pltpu.VMEM((steps, chunk, depth), F32),
            pltpu.VMEM((steps, total + 2 * front, depth), F32),
            pltpu.VMEM((steps, total + 2 * front, depth), F32),
            pltpu.VMEM((steps * block, depth), F32),
            square,
            far[0],
            wide,
            wide,
            wide,
            *far[3:],
            pltpu.SemaphoreType.DMA((7,)),
        ],
        10**9,
        middle, left, right, bundle,
        limit=VMEM_BYTES - room,
    )[0]
    arrived = exchanged(back).reshape(steps, columns, block, depth)
    return jnp.transpose(arrived, (1, 0, 2, 3)).reshape(1, columns, size, depth)


def solution(mesh):
    return jax.shard_map(
        correction,
        mesh=mesh,
        in_specs=(
            P("tm", "tx", None, None),
            P("tm", "tx", None, None),
            P("tx", None, None),
            P("tx", None),
            P(),
            P(),
        ),
        out_specs=P("tm", "tx", None, None),
        check_vma=False,
    )
```

```python
import functools

import jax
import jax.numpy as jnp
from jax import lax
from jax.experimental import pallas as pl
from jax.experimental.pallas import tpu as pltpu
from jax.sharding import PartitionSpec as P


ALPHA = 0.05
REACH = 2
F32 = jnp.float32
BF16 = jnp.bfloat16
MIB = 2**20
VMEM_BYTES = 67043328


def split(value):
    high = value.astype(BF16)
    return high, (value - high.astype(F32)).astype(BF16)


def dot(left, right):
    return jnp.dot(left, right, preferred_element_type=F32)


def shifted(array, axis, by):
    count = lax.axis_size(axis)
    pairs = [(i, i + by) for i in range(count) if 0 <= i + by < count]
    return lax.ppermute(array, axis, pairs)


def cut(value, rows, out, base, blocks):
    size = value.shape[0]
    block = size // blocks
    tall = block + 2 * REACH
    rows[pl.ds(REACH, size), :] = value
    for target in range(blocks):
        out[target, pl.ds(base, tall), :] = rows[pl.ds(block * target, tall), :]


def fill_weights(weights, first_half, second_half):
    depth = first_half.shape[0]
    first_high, first_low = split(first_half)
    weights[:depth, :depth] = first_high
    weights[:depth, depth:] = first_low
    if second_half is None:
        weights[depth:, :depth] = first_high
        weights[depth:, depth:] = jnp.zeros_like(first_low)
    else:
        second_high, second_low = split(second_half)
        weights[depth:, :depth] = second_high
        weights[depth:, depth:] = second_low


def times_matrix(value, weights):
    depth = value.shape[1]
    wide = dot(jnp.concatenate(split(value), axis=1), weights[...])
    return wide[:, :depth] + wide[:, depth:]


def pack_kernel(block, count, mine, other, *rest):
    outs, windows, loads = rest[:count], rest[count], rest[count + 1]
    columns, size, _ = mine.shape
    broad = windows.shape[2]
    tall = block + 2 * REACH
    here = lax.axis_index("tm")
    odd = here % 2 == 1
    targets = [(here + 2 * by) % (size // block) for by in range(1, count + 1)]
    begins = [pl.multiple_of(near_begin(target, block, broad, size), 8) for target in targets]

    def load(source, by):
        return pltpu.make_async_copy(source.at[:, pl.ds(begins[by], broad), :], windows.at[by], loads.at[by])

    @pl.when(odd)
    def _():
        for by in range(count):
            load(mine, by).start()

    @pl.when(jnp.logical_not(odd))
    def _():
        for by in range(count):
            load(other, by).start()

    for by in range(count):
        load(mine, by).wait()

    def pair(step, carry):
        base = pl.multiple_of(step * 2 * tall, 8)
        for by in range(count):
            take = pl.ds(window_start(targets[by], block, tall, size) - begins[by], tall)
            for which in range(2):
                outs[by][pl.ds(base + which * tall, tall), :] = windows[by, 2 * step + which, take, :]
        return carry

    lax.fori_loop(0, columns // 2, pair, 0)


def residual_kernel(
    blocks, inner, state, other, initial, force, low, high, kappa, rates, basis, out,
    here, past, pushed, parts, rows, levels, turned, weights, sides, plain_ref, rates_ref, loads, stores, extras,
):
    columns, size, depth = state.shape
    tall = size // blocks + 2 * REACH
    step_here = lax.axis_index("tm")
    odd = step_here % 2 == 1
    first = step_here == 0
    if inner:
        group = 4 if (columns - 4) % 4 == 0 else 2
        count = (columns - 4) // group
        spans = [(2 + group * step, group) for step in range(count)]
        wide = [(1 if step == 0 else start + 1, group + 2 if step == 0 else group) for step, (start, _) in enumerate(spans)]
    else:
        group = 2
        count = 2
        spans = [(0, 2), (columns - 2, 2)]
        wide = [(0, 3), (columns - 3, 3)]

    def load(kind, step, source=None):
        start, extent = (wide if kind == 0 else spans)[step]
        take = pl.ds(start, extent)
        source = (state, other, force)[kind] if source is None else source
        target = here.at[take, pl.ds(8, size), :] if kind == 0 else (past, pushed)[kind - 1].at[take]
        return pltpu.make_async_copy(source.at[take], target, loads.at[kind, step])

    def arrive(step):
        start = pl.ds(0, group)
        pltpu.make_async_copy(force.at[start], pushed.at[start], loads.at[2, step]).wait()
        if inner:
            pltpu.make_async_copy(state.at[start], here.at[start, pl.ds(8, size), :], loads.at[0, step]).wait()

        @pl.when(jnp.logical_or(odd, first))
        def _():
            pltpu.make_async_copy(other.at[start], past.at[start], loads.at[1, step]).wait()

    def level(x):
        return here[x, pl.ds(8, size), :]

    small = [(basis, plain_ref), (rates, rates_ref), (kappa, levels.at[pl.ds(0, columns), :])]
    if not inner:
        small += [(low, sides.at[0]), (high, sides.at[1])]
    small = [pltpu.make_async_copy(*ends, extras.at[i]) for i, ends in enumerate(small)]
    levels[...] = jnp.zeros_like(levels)
    for copy in small:
        copy.start()
    for step in range(count):
        load(0, step).start()
        load(2, step).start()

    @pl.when(odd)
    def _():
        for step in range(count):
            load(1, step).start()

    @pl.when(first)
    def _():
        for step in range(count):
            load(1, step, initial).start()

    here[:, :8, :] = jnp.zeros((columns, 8, depth), F32)
    here[:, 8 + size :, :] = jnp.zeros((columns, 8, depth), F32)

    rows[...] = jnp.zeros_like(rows)
    for copy in small:
        copy.wait()
    plain = plain_ref[...]
    fill_weights(weights, plain, -plain * rates_ref[...])
    for part in range(size // depth):
        where = pl.ds(part * depth, depth)
        turned[where, :] = jnp.transpose(levels[:, where])

    def residual(x, left, right, across):
        center = level(x)
        square = center * center
        beside = left + right + here[x, pl.ds(7, size), :] + here[x, pl.ds(9, size), :]
        return (
            pushed[x]
            - center
            + jnp.where(jnp.logical_or(odd, first), past[x], 0.0)
            - across * (4.0 * center - beside)
            - 0.5 * (square * center) / (1.0 + square)
        )

    def columns_of(x, group, sides_of, base):
        rolled = turned[...] if isinstance(x, int) else pltpu.roll(turned[...], depth - x, 1)
        at = x if isinstance(x, int) else 0
        for begin in range(0, group, 2):
            highs, lows = [], []
            for which in range(begin, begin + 2):
                across = jnp.broadcast_to(rolled[:, at + which : at + which + 1], (size, depth))
                value_high, value_low = split(residual(x + which, *sides_of(x + which), across))
                center_high, center_low = split(level(x + which))
                highs.append(jnp.concatenate([value_high, center_high], axis=1))
                lows.append(jnp.concatenate([value_low, center_low], axis=1))
            product = dot(jnp.concatenate(highs, axis=0), weights[...])
            modal = product[:, :depth] + product[:, depth:] + dot(jnp.concatenate(lows, axis=0), weights[:, :depth])
            for which in range(2):
                part = modal[which * size : (which + 1) * size]
                cut(part, rows.at[begin + which], parts, base + (begin + which) * tall, blocks)

    def store(step):
        where = pl.ds(pl.multiple_of(step * group * tall, 8), group * tall)
        return pltpu.make_async_copy(parts.at[:, where, :], out.at[:, where, :], stores.at[step])

    if inner:
        pair_of = pl.ds(0, 2)
        pltpu.make_async_copy(state.at[pair_of], here.at[pair_of, pl.ds(8, size), :], loads.at[0, 0]).wait()

        def pair(step, carry):
            base = pl.multiple_of(step * group * tall, 8)
            x = 2 + group * step
            arrive(step)
            columns_of(x, group, lambda at: (level(at - 1), level(at + 1)), base)
            store(step).start()
            return carry

        lax.fori_loop(0, count, pair, 0)
    else:
        for step in range(count):
            load(0, step).wait()
            arrive(step)
        columns_of(0, 2, lambda at: (sides[0] if at == 0 else level(0), level(at + 1)), 0)
        store(0).start()
        last = columns - 1
        columns_of(last - 1, 2, lambda at: (level(at - 1), sides[1] if at == last else level(last)), 2 * tall)
        store(1).start()
    for step in range(count):
        store(step).wait()


def modes_kernel(block, count, spans, edge, state, other, kappa, rates, basis, *rest):
    pieces = rest[:count]
    first_out, second_out, third_out, near, far, strip, gathered, weights, plain_ref, rates_ref, edges, cells, loads, stores = rest[count:]
    broad, _ = near.shape[1:]
    chips = count + 1
    steps = 2 * chips
    size = block * steps
    tall = block + 2 * REACH
    room = (strip.shape[1] - broad) // 2
    here = lax.axis_index("tm")
    chip = here // 2
    odd = here % 2 == 1
    width = sum(stop - start for start, stop in spans)
    near_start = pl.multiple_of(near_begin(here, block, broad, size), 8)

    def copies(source):
        made = []
        at = 0
        for start, stop in spans:
            take = pl.ds(start, stop - start)
            put = pl.ds(at, stop - start)
            made.append((source.at[take, pl.ds(near_start, broad), :], near.at[put]))
            flat, into = pl.ds(start * tall, (stop - start) * tall), pl.ds(at * tall, (stop - start) * tall)
            made += [(pieces[by].at[flat, :], far.at[by, into, :]) for by in range(count)]
            at += stop - start
        return [pltpu.make_async_copy(*ends, loads.at[i]) for i, ends in enumerate(made)]

    small = [(basis, plain_ref), (rates, rates_ref), (kappa, cells)]
    if edge is not None:
        small.append((edge, edges))
    small = [pltpu.make_async_copy(*ends, stores.at[i]) for i, ends in enumerate(small)]

    @pl.when(odd)
    def _():
        for copy in copies(state):
            copy.start()

    @pl.when(jnp.logical_not(odd))
    def _():
        for copy in copies(other):
            copy.start()

    for copy in small:
        copy.start()
    strip[...] = jnp.zeros_like(strip)
    for copy in small:
        copy.wait()
    fill_weights(weights, plain_ref[...], None)
    if edge is None:
        chunk = 2 * tall

        def factors(step, carry):
            base = pl.multiple_of(step * chunk, 8)
            second_out[pl.ds(base, chunk), :], third_out[pl.ds(base, chunk), :] = time_factors(
                cells[pl.ds(base, chunk), :], rates_ref[...], steps
            )
            return carry

        lax.fori_loop(0, cells.shape[0] // chunk, factors, 0)
    for copy in copies(state):
        copy.wait()
    begin = block * here - REACH + room

    def keep(slot, value):
        first_out[pl.ds(pl.multiple_of(slot * (width * tall), 8), width * tall), :] = value

    def gather(source, start, extent):
        for x in range(width):
            strip[x % 2, pl.ds(room, extent), :] = source(x)
            gathered[pl.ds(x * tall, tall), :] = strip[x % 2, pl.ds(begin - start, tall), :]
        return times_matrix(gathered[...], weights)

    keep(chip, gather(lambda x: near[x], near_start, broad))

    far_start = window_start(here, block, tall, size)
    strip[...] = jnp.zeros_like(strip)

    def far_slot(by, carry):
        keep((chip - by - 1 + chips) % chips, gather(lambda x: far[by, pl.ds(x * tall, tall), :], far_start, tall))
        return carry

    lax.fori_loop(0, count, far_slot, 0)
    if edge is not None:
        two = REACH * tall
        for n in range(steps):
            left = edges[n, :two, :]
            right = edges[n, two:, :]
            if n and n % 2 == 0:
                at = (n // 2 - 1) * 2 * two
                left = left + first_out[at : at + two, :]
                right = right + first_out[at + two : at + 2 * two, :]
            second_out[n * two : (n + 1) * two, :] = left
            third_out[n * two : (n + 1) * two, :] = right
        second_out[steps * two :, :] = cells[:two, :]
        third_out[steps * two :, :] = cells[cells.shape[0] - two :, :]


def time_factors(kappa, rates, steps):
    inverse = 1.0 / (1.0 + rates + 4.0 * kappa)
    power = inverse
    for _ in range(steps - 1):
        power = power * inverse
    return inverse, ALPHA / (1.0 - ALPHA * power)


def rim_kernel(block, count, spans, edge, state, other, kappa, rates, basis, *rest):
    outs, scratch = rest[count : count + 2], rest[count + 2 :]
    modes_kernel(block, count, spans, edge, state, other, kappa, rates, basis, *rest[:count], scratch[0], *outs, *scratch[1:])


def fill_kernel(block, count, spans, state, other, edge_low, edge_high, kappa, rates, basis, *rest):
    bundle, scratch = rest[count], rest[count + 1 :]
    modal, inverse, ending, ends, turned, sems = scratch[:6]
    sides = [pltpu.make_async_copy(edge, ends.at[i], sems.at[i]) for i, edge in enumerate((edge_low, edge_high))]
    for copy in sides:
        copy.start()
    inner = scratch[6:]
    modes_kernel(block, count, spans, None, state, other, kappa, rates, basis, *rest[:count], modal, inverse, ending, *inner)
    plain_ref, rates_ref, cells = inner[5], inner[6], inner[8]
    turned[pl.ds(0, plain_ref.shape[0]), :] = jnp.transpose(plain_ref[...])
    turned[pl.ds(plain_ref.shape[0], 8), :] = jnp.broadcast_to(rates_ref[...], (8, plain_ref.shape[1]))
    for copy in sides:
        copy.wait()
    copies = [
        pltpu.make_async_copy(source, bundle.at[pl.ds(start, source.shape[0]), :], sems.at[2 + i])
        for i, (source, start) in enumerate(bundle_parts(modal, cells, inverse, ending, ends, turned))
    ]
    for copy in copies:
        copy.start()
    for copy in copies:
        copy.wait()


def bundle_parts(modal, cells, inverse, ending, ends, turned):
    placed = []
    at = 0
    for part in (cells, inverse, ending, ends.at[0], ends.at[1], turned, modal):
        placed.append((part, at))
        at += part.shape[0]
    return placed


def relax_kernel(
    block, middle, left, right, bundle, out,
    known, source, older, newer, gathered, weights, modal, kappa, inverse, ending, ends, turned, loads,
):
    steps, inner, depth = middle.shape
    tall = block + 2 * REACH
    chunk = REACH * tall
    columns = inner // tall + 2 * REACH
    total = inner + 4 * chunk
    pad = older.shape[1] - total
    front = pad // 2
    own = pl.ds(chunk, total - 2 * chunk)
    parts = bundle_parts(modal, kappa.at[own, :], inverse.at[own, :], ending.at[own, :], ends, turned)
    copies = [
        pltpu.make_async_copy(bundle.at[pl.ds(start, target.shape[0]), :], target, loads.at[i])
        for i, (target, start) in enumerate(parts)
    ]
    for copy in copies:
        copy.start()
    older[:, :front, :] = jnp.zeros((steps, front, depth), F32)
    older[:, front + total :, :] = jnp.zeros((steps, pad - front, depth), F32)
    for ghost, base in ((left, 0), (right, total - chunk)):
        kappa[pl.ds(base, chunk), :] = ghost[steps * chunk :, :]
    copies[5].wait()
    fill_weights(weights, turned[:depth, :], None)
    for base in (0, total - chunk):
        at = pl.ds(base, chunk)
        inverse[at, :], ending[at, :] = time_factors(kappa[at, :], turned[depth : depth + 1, :], steps)

    def solve(values, inv, end):
        last = values(0) * inv
        for n in range(1, steps):
            last = (values(n) + last) * inv
        return end * last

    def first(value, base):
        inv = inverse[pl.ds(base, chunk), :]
        run = solve(value, inv, ending[pl.ds(base, chunk), :])
        for n in range(steps):
            run = (known[n, pl.ds(base, chunk), :] + run) * inv
            older[n, pl.ds(base + front, chunk), :] = run

    def keep(value, base):
        def kept(n):
            made = value(n)
            known[n, pl.ds(base, chunk), :] = made
            return made

        return kept

    first(keep(lambda n: left[n * chunk : (n + 1) * chunk, :], 0), 0)
    first(keep(lambda n: right[n * chunk : (n + 1) * chunk, :], total - chunk), total - chunk)
    for copy in copies[:5]:
        copy.wait()
    first(keep(lambda n: ends[0, n * chunk : (n + 1) * chunk, :], chunk), chunk)
    first(keep(lambda n: ends[1, n * chunk : (n + 1) * chunk, :], total - 2 * chunk), total - 2 * chunk)
    copies[6].wait()

    def first_middle(step, carry):
        at = pl.multiple_of(step * chunk, 8)
        base = pl.multiple_of(at + 2 * chunk, 8)

        def value(n):
            made = middle[n, pl.ds(at, chunk), :]
            if n and n % 2 == 0:
                made = made + modal[pl.ds((n // 2 - 1) * inner + at, chunk), :]
            return made

        first(keep(value, base), base)
        return carry

    lax.fori_loop(0, inner // chunk, first_middle, 0)

    def term(field, base, size, n):
        beside = (
            field[n, pl.ds(base + front - 1, size), :]
            + field[n, pl.ds(base + front + 1, size), :]
            + field[n, pl.ds(base + front - tall, size), :]
            + field[n, pl.ds(base + front + tall, size), :]
        )
        return known[n, pl.ds(base, size), :] + kappa[pl.ds(base, size), :] * beside

    def second(step, carry):
        base = pl.multiple_of(step * chunk, 8) + tall
        inv = inverse[pl.ds(base, chunk), :]

        def value(n):
            made = term(older, base, chunk, n)
            source[n, :chunk, :] = made
            return made

        run = solve(value, inv, ending[pl.ds(base, chunk), :])
        for n in range(steps):
            run = (source[n, :chunk, :] + run) * inv
            newer[n, pl.ds(base + front, chunk), :] = run
        return carry

    lax.fori_loop(0, (columns + 2) // 2, second, 0)

    def third(base, which):
        inv = inverse[pl.ds(base, block), :]
        rows = pl.ds(which * block, block)

        def value(n):
            made = term(newer, base, block, n)
            source[n, rows, :] = made
            return made

        run = solve(value, inv, ending[pl.ds(base, block), :])
        for n in range(steps):
            run = (source[n, rows, :] + run) * inv
            gathered[pl.ds((which * steps + n) * block, block), :] = run

    def third_pair(step, carry):
        at = pl.multiple_of(step * 2 * tall, 8)
        to = pl.multiple_of(step * 2 * block, 8)
        for which in range(2):
            third(at + chunk + which * tall + REACH, which)
        gathered[...] = times_matrix(gathered[...], weights)
        for which in range(2):
            for n in range(steps):
                part = gathered[pl.ds((which * steps + n) * block, block), :]
                out[n, pl.ds(to + which * block, block), :] = part
        return carry

    lax.fori_loop(0, columns // 2, third_pair, 0)


SPACES = {"v": pltpu.VMEM, "h": pltpu.HBM}


def call(kernel, outs, spaces, scratch, flops, *operands, limit=None):
    shapes = [jax.ShapeDtypeStruct(shape, F32) for shape, _ in outs]
    return pl.pallas_call(
        kernel,
        out_shape=shapes,
        in_specs=[pl.BlockSpec(memory_space=SPACES[space]) for space in spaces],
        out_specs=[pl.BlockSpec(memory_space=SPACES[space]) for _, space in outs],
        scratch_shapes=scratch,
        cost_estimate=pl.CostEstimate(flops=flops, bytes_accessed=10**6, transcendentals=0),
        compiler_params=pltpu.CompilerParams(vmem_limit_bytes=60 * MIB if limit is None else limit),
    )(*operands)


def paired(array):
    count = lax.axis_size("tm")
    return lax.ppermute(array, "tm", [(i, i ^ 1) for i in range(count)])


def exchanged(array):
    return lax.all_to_all(array, "tm", split_axis=0, concat_axis=0, tiled=True)


def near_begin(device, block, broad, size):
    return jnp.clip((block * device - REACH) // 8 * 8, 0, size - broad)


def window_start(device, block, window, size):
    return jnp.clip(block * device - REACH, 0, size - window)


def spread(rows, by):
    count = lax.axis_size("tm")
    return lax.ppermute(rows, "tm", [(i, (i + 2 * by) % count) for i in range(count - 2)])


def correction(state, force, u_init, kappa, rates, basis):
    steps = lax.axis_size("tm")
    here = lax.axis_index("tm")
    chips = steps // 2
    columns, size, depth = u_init.shape
    block = size // steps
    tall = block + 2 * REACH
    chunk = REACH * tall
    broad = (block + 23) // 8 * 8
    inside = columns - 2 * REACH
    total = columns * tall + 2 * chunk
    front = (tall + 15) // 8 * 8
    square = pltpu.VMEM((2 * depth, 2 * depth), BF16)
    constants = [pltpu.VMEM((depth, depth), F32), pltpu.VMEM((1, depth), F32)]
    mine = state[0]
    other = paired(mine)
    low = shifted(mine[-1], "tx", 1)
    high = shifted(mine[0], "tx", -1)
    rates_row = rates.reshape(1, depth)
    packed = call(
        functools.partial(pack_kernel, block, chips - 1),
        [((columns * tall, depth), "v")] * (chips - 1),
        "hh",
        [pltpu.VMEM((chips - 1, columns, broad, depth), F32), pltpu.SemaphoreType.DMA((chips - 1,))],
        10**7,
        mine, other,
    )
    pieces = []
    for by in range(1, chips):
        pieces.append(spread(packed[by - 1], by))

    def residual(inner, count, flops):
        return call(
            functools.partial(residual_kernel, steps, inner),
            [((steps, count * tall, depth), "h")],
            "hhhhhhhhh",
            [
                pltpu.VMEM((columns, size + 16, depth), F32),
                pltpu.VMEM(u_init.shape, F32),
                pltpu.VMEM(u_init.shape, F32),
                pltpu.VMEM((steps, count * tall, depth), F32),
                pltpu.VMEM((4, size + 8, depth), F32),
                pltpu.VMEM((depth, size), F32),
                pltpu.VMEM((size, depth), F32),
                square,
                pltpu.VMEM((2, size, depth), F32),
                *constants,
                pltpu.SemaphoreType.DMA((3, max(count // 4, 2) if count % 4 == 0 else count // 2)),
                pltpu.SemaphoreType.DMA((max(count // 4, 2) if count % 4 == 0 else count // 2,)),
                pltpu.SemaphoreType.DMA((3 if inner else 5,)),
            ],
            flops,
            mine, other, u_init, force[0], low, high, kappa, rates_row, basis,
        )[0]

    edge = residual(False, 2 * REACH, 2 * 10**9)
    edge = exchanged(edge)
    middle = residual(True, columns - 2 * REACH, 6 * 10**9)
    middle = exchanged(middle)
    kappa_wide = jnp.pad(kappa, ((0, 0), (REACH, REACH)))
    kappa_mine = lax.dynamic_slice_in_dim(kappa_wide, here * block, tall, 1)
    kappa_cells = jnp.broadcast_to(kappa_mine[:, :, None], kappa_mine.shape + (depth,)).reshape(-1, depth)

    def modes_scratch(width):
        return [
            pltpu.VMEM((width, broad, depth), F32),
            pltpu.VMEM((chips - 1, width * tall, depth), F32),
            pltpu.VMEM((2, broad + 32, depth), F32),
            pltpu.VMEM((width * tall, depth), F32),
            square,
            *constants,
            pltpu.VMEM((steps, 2 * chunk, depth), F32),
            pltpu.VMEM((columns * tall, depth), F32),
            pltpu.SemaphoreType.DMA((2 * chips,)),
            pltpu.SemaphoreType.DMA((4,)),
        ]

    edge_low, edge_high = call(
        functools.partial(rim_kernel, block, chips - 1, [(0, REACH), (columns - REACH, columns)]),
        [(((steps + 1) * chunk, depth), "v")] * 2,
        "h" * (5 + chips),
        [pltpu.VMEM((chips * 2 * chunk, depth), F32)] + modes_scratch(2 * REACH),
        10**9,
        edge, mine, other, kappa_cells, rates_row, basis, *pieces,
    )
    left = shifted(edge_high, "tx", 1)
    right = shifted(edge_low, "tx", -1)
    far = [
        pltpu.VMEM((chips * inside * tall, depth), F32),
        pltpu.VMEM((columns * tall, depth), F32),
        pltpu.VMEM((columns * tall, depth), F32),
        pltpu.VMEM((2, (steps + 1) * chunk, depth), F32),
        pltpu.VMEM((depth + 8, depth), F32),
    ]
    rows = chips * inside * tall + 3 * columns * tall + 2 * (steps + 1) * chunk + depth + 8
    room = 16 * (middle.size + 2 * left.size + u_init.size)
    rows = max(rows, -(-(room + MIB) // (4096 * depth)) * 1024)
    bundle = call(
        functools.partial(fill_kernel, block, chips - 1, [(REACH, columns - REACH)]),
        [((rows, depth), "h")],
        "h" * (6 + chips),
        far + [pltpu.SemaphoreType.DMA((9,))] + modes_scratch(inside),
        10**9,
        mine, other, edge_low, edge_high, kappa_cells, rates_row, basis, *pieces,
    )[0]
    wide = pltpu.VMEM((total, depth), F32)
    back = call(
        functools.partial(relax_kernel, block),
        [((steps, columns * block, depth), "v")],
        "vvvh",
        [
            pltpu.VMEM((steps, total, depth), F32),
            pltpu.VMEM((steps, chunk, depth), F32),
            pltpu.VMEM((steps, total + 2 * front, depth), F32),
            pltpu.VMEM((steps, total + 2 * front, depth), F32),
            pltpu.VMEM((2 * steps * block, depth), F32),
            square,
            far[0],
            wide,
            wide,
            wide,
            *far[3:],
            pltpu.SemaphoreType.DMA((7,)),
        ],
        10**9,
        middle, left, right, bundle,
        limit=VMEM_BYTES - room,
    )[0]
    arrived = exchanged(back).reshape(steps, columns, block, depth)
    return jnp.transpose(arrived, (1, 0, 2, 3)).reshape(1, columns, size, depth)


def solution(mesh):
    return jax.shard_map(
        correction,
        mesh=mesh,
        in_specs=(
            P("tm", "tx", None, None),
            P("tm", "tx", None, None),
            P("tx", None, None),
            P("tx", None),
            P(),
            P(),
        ),
        out_specs=P("tm", "tx", None, None),
        check_vma=False,
    )
```
